128 devices in a mesh: data: 128 (over z, y, x, core).
Axes of the slice: x: 4, y: 4, z: 4, core: 2. Of those that a mesh axis runs over, the one named last changes fastest.
Arguments:
- tokens: bfloat16 [262144, 1024], P('data')
- w_up: bfloat16 [1024, 4096], replicated
- w_down: bfloat16 [4096, 1024], replicated
- heads: bfloat16 [4, 1024, 3], replicated
- labels: int32 [4, 262144], P(None, 'data')
Outputs:
- output 1: float32 [4], replicated
- output 2: float32 [1024, 4096], P('data')
- output 3: float32 [4096, 1024], P('data')
All inputs are finite; a program needn't handle non-finite values.
Results may differ from the reference program's by a relative error of at most 0.001.
Values are sent between devices in bfloat16 or wider.
A program may use at most 1 GiB of HBM per device.

```python
import jax
import jax.numpy as jnp
from jax import lax

MODEL_DIM = 1024
HIDDEN_DIM = 4096
NUM_TASKS = 4
NUM_CLASSES = 3
TOKENS_DEV = 2048
GROUP_SIZE = 128
SOLVER_STEPS = 20


def draw_labels(label_key):
    label_keys = jax.random.split(label_key, 4)
    total_rows = TOKENS_DEV * GROUP_SIZE
    spread = (NUM_CLASSES + 1) // 2
    offsets = jax.random.randint(label_keys[0], (GROUP_SIZE,), 0, NUM_CLASSES)
    shared = (jnp.repeat(offsets, TOKENS_DEV) + jax.random.randint(label_keys[1], (total_rows,), 0, spread)) % NUM_CLASSES
    keep_mask = jax.random.randint(label_keys[2], (NUM_TASKS, total_rows), 0, 10) < 7
    own_labels = jax.random.randint(label_keys[3], (NUM_TASKS, total_rows), 0, NUM_CLASSES)
    return jnp.where(keep_mask, shared[None, :], own_labels).astype(jnp.int32)


def setup_inputs(seed: int = 0) -> dict:
    root_key = jax.random.key(seed)
    sub_keys = jax.random.split(root_key, 7)
    total_rows = TOKENS_DEV * GROUP_SIZE
    tokens = jax.random.normal(sub_keys[0], (total_rows, MODEL_DIM), jnp.float32)
    w_up = jax.random.normal(sub_keys[1], (MODEL_DIM, HIDDEN_DIM), jnp.float32) * MODEL_DIM ** -0.5
    w_down = jax.random.normal(sub_keys[2], (HIDDEN_DIM, MODEL_DIM), jnp.float32) * HIDDEN_DIM ** -0.5
    shared_head = jax.random.normal(sub_keys[3], (1, MODEL_DIM, NUM_CLASSES), jnp.float32)
    own_head = jax.random.normal(sub_keys[4], (NUM_TASKS, MODEL_DIM, NUM_CLASSES), jnp.float32)
    task_scale = jax.random.uniform(sub_keys[5], (NUM_TASKS, 1, 1), jnp.float32, 0.7, 1.3)
    signs = (1 - 2 * (jnp.arange(NUM_TASKS) % 2)).astype(jnp.float32).reshape(NUM_TASKS, 1, 1)
    heads = task_scale * (0.8 * signs * shared_head + 0.6 * own_head) * MODEL_DIM ** -0.5
    labels = draw_labels(sub_keys[6])
    return {'tokens': tokens.astype(jnp.bfloat16), 'w_up': w_up.astype(jnp.bfloat16), 'w_down': w_down.astype(jnp.bfloat16), 'heads': heads.astype(jnp.bfloat16), 'labels': labels}


def trunk_forward(x_rows, w_up, w_down):
    pre_act = jnp.dot(x_rows, w_up, preferred_element_type=jnp.float32).astype(jnp.bfloat16)
    hidden = jax.nn.gelu(pre_act.astype(jnp.float32)).astype(jnp.bfloat16)
    trunk_out = x_rows.astype(jnp.float32) + jnp.dot(hidden, w_down, preferred_element_type=jnp.float32)
    return pre_act, hidden, trunk_out


def task_residuals(trunk_out, heads_f32, label_rows, total_rows):
    logits = jnp.einsum('bd,tdc->tbc', trunk_out.astype(jnp.bfloat16).astype(jnp.float32), heads_f32)
    onehot = (label_rows[:, :, None] == jnp.arange(NUM_CLASSES)[None, None, :]).astype(jnp.float32)
    return (jax.nn.softmax(logits, axis=-1) - onehot) / total_rows


def solve_weights(full_gram):
    step_scale = jnp.trace(full_gram) / NUM_TASKS

    def update(step_idx, mix_wts):
        descent = jnp.sum(full_gram * mix_wts[None, :], axis=1)
        mix_wts = mix_wts * jnp.exp(-descent / step_scale)
        return mix_wts / jnp.sum(mix_wts)

    uniform_start = jnp.full((NUM_TASKS,), 1.0 / NUM_TASKS, jnp.float32)
    return lax.fori_loop(0, SOLVER_STEPS, update, uniform_start)


def reference(tokens, w_up, w_down, heads, labels):
    total_rows = tokens.shape[0]
    num_blocks = total_rows // TOKENS_DEV
    tok_blocks = tokens.reshape(num_blocks, TOKENS_DEV, MODEL_DIM)
    lab_blocks = labels.reshape(NUM_TASKS, num_blocks, TOKENS_DEV).transpose(1, 0, 2)
    heads_f32 = heads.astype(jnp.float32)
    head_gram = jnp.einsum('tdc,sde->tcse', heads_f32, heads_f32)

    def gram_step(gram_acc, block_in):
        x_rows, label_rows = block_in
        trunk_out = trunk_forward(x_rows, w_up, w_down)[2]
        task_resid = task_residuals(trunk_out, heads_f32, label_rows, total_rows)
        res_outer = jnp.einsum('tbc,sbe->tcse', task_resid, task_resid)
        return gram_acc + jnp.sum(res_outer * head_gram, axis=(1, 3)), None

    full_gram, _ = lax.scan(gram_step, jnp.zeros((NUM_TASKS, NUM_TASKS), jnp.float32), (tok_blocks, lab_blocks))
    mix_weights = solve_weights(full_gram)

    def grad_step(grad_acc, block_in):
        x_rows, label_rows = block_in
        pre_act, hidden, trunk_out = trunk_forward(x_rows, w_up, w_down)
        task_resid = task_residuals(trunk_out, heads_f32, label_rows, total_rows)
        d_out = jnp.einsum('tbc,tdc->bd', task_resid * mix_weights[:, None, None], heads_f32).astype(jnp.bfloat16)
        grad_down = jnp.dot(hidden.T, d_out, preferred_element_type=jnp.float32)
        d_hidden = jnp.dot(d_out, w_down.T, preferred_element_type=jnp.float32)
        gelu_vjp = jax.vjp(jax.nn.gelu, pre_act.astype(jnp.float32))[1]
        d_pre = gelu_vjp(d_hidden)[0].astype(jnp.bfloat16)
        grad_up = jnp.dot(x_rows.T, d_pre, preferred_element_type=jnp.float32)
        return (grad_acc[0] + grad_up, grad_acc[1] + grad_down), None

    zero_grads = (jnp.zeros((MODEL_DIM, HIDDEN_DIM), jnp.float32), jnp.zeros((HIDDEN_DIM, MODEL_DIM), jnp.float32))
    (grad_up, grad_down), _ = lax.scan(grad_step, zero_grads, (tok_blocks, lab_blocks))
    return mix_weights, grad_up, grad_down
```

```python
import functools

import jax
import jax.numpy as jnp
from jax import lax
from jax.experimental import pallas as pl
from jax.experimental.pallas import tpu as pltpu
from jax.sharding import PartitionSpec as P

SOLVER_STEPS = 20
EXACT_PREC = lax.Precision.HIGHEST
MESH = pl.DeviceIdType.MESH
VMEM_BYTES = 67_043_328
ROWS = 8


def coords(me):
    return me % 2, (me // 2) % 4, (me // 8) % 4, me // 32


def axis_of(k, x, y, z):
    wz = (k - 1) * (k - 2) // 2
    wy = k * (2 - k)
    wx = k * (k - 1) // 2
    return z * wz + y * wy + x * wx, 32 * wz + 8 * wy + 2 * wx


def enter(peers):
    barrier = pltpu.get_barrier_semaphore()
    for peer in peers:
        pl.semaphore_signal(barrier, inc=1, device_id=(peer,), device_id_type=MESH)
    pl.semaphore_wait(barrier, len(peers))


def gram_kernel(gram_ref, wts_ref, stage0, stage1, stage2, tot0, tot1, send_sem, recv_sem):
    me = lax.axis_index('data')
    c, x, y, z = coords(me)
    low = me % 8
    group0 = [me - low + (low + d) % 8 for d in range(1, 8)]
    group1 = [me + ((y + d) % 4 - y) * 8 for d in range(1, 4)]
    group2 = [me + ((z + d) % 4 - z) * 32 for d in range(1, 4)]
    enter(group0 + group1 + group2)

    def exchange(src, slots, slot, group, first):
        copies = []
        for n, peer in enumerate(group):
            copy = pltpu.make_async_remote_copy(
                src_ref=src,
                dst_ref=slots.at[slot],
                send_sem=send_sem.at[first + n],
                recv_sem=recv_sem.at[first + n],
                device_id=(peer,),
                device_id_type=MESH,
            )
            copy.start()
            copies.append(copy)
        slots[slot] = src[...]
        for copy in copies:
            copy.wait()

    exchange(gram_ref, stage0, low, group0, 0)
    tot0[...] = sum(stage0[n] for n in range(1, 8)) + stage0[0]
    exchange(tot0, stage1, y, group1, 7)
    tot1[...] = (stage1[0] + stage1[1]) + (stage1[2] + stage1[3])
    exchange(tot1, stage2, z, group2, 10)
    full = (stage2[0] + stage2[1]) + (stage2[2] + stage2[3])
    gram, gram_t = full[0], full[1]
    row = lax.broadcasted_iota(jnp.int32, gram.shape, 0)
    lane = lax.broadcasted_iota(jnp.int32, gram.shape, 1)
    trace = jnp.sum(jnp.where(row == lane, gram, 0.0), axis=(0, 1), keepdims=True)
    scale = jnp.broadcast_to(trace / 4, gram.shape)
    by_lane = jnp.where(lane < 4, 0.25, 0.0)
    by_row = jnp.where(row < 4, 0.25, 0.0)
    for _ in range(SOLVER_STEPS):
        down_row = jnp.sum(gram * by_lane, axis=1, keepdims=True)
        down_lane = jnp.sum(gram_t * by_row, axis=0, keepdims=True)
        by_row = by_row * jnp.exp(-down_row / scale)
        by_lane = by_lane * jnp.exp(-down_lane / scale)
        by_row = by_row / jnp.sum(by_row, axis=0, keepdims=True)
        by_lane = by_lane / jnp.sum(by_lane, axis=1, keepdims=True)
    wts_ref[...] = by_lane


def solve_weights(part_gram):
    pads = ((0, 0), (0, 4), (0, 124))
    both = jnp.pad(jnp.stack([part_gram, part_gram.T]), pads)
    wts = pl.pallas_call(
        gram_kernel,
        out_shape=jax.ShapeDtypeStruct((8, 128), jnp.float32),
        in_specs=[pl.BlockSpec(memory_space=pltpu.VMEM)],
        out_specs=pl.BlockSpec(memory_space=pltpu.VMEM),
        scratch_shapes=[
            pltpu.VMEM((8, 2, 8, 128), jnp.float32),
            pltpu.VMEM((4, 2, 8, 128), jnp.float32),
            pltpu.VMEM((4, 2, 8, 128), jnp.float32),
            pltpu.VMEM((2, 8, 128), jnp.float32),
            pltpu.VMEM((2, 8, 128), jnp.float32),
            pltpu.SemaphoreType.DMA((13,)),
            pltpu.SemaphoreType.DMA((13,)),
        ],
        compiler_params=pltpu.CompilerParams(collective_id=0, has_side_effects=True),
    )(both)
    return wts[0, :4]


def scatter_kernel(n_down, n_up, width, down_ref, up_ref, out_down, out_up, src, pair_in, work, opp_r, opp_l, from_l, from_r,
                   mid, mid_in, low, low_in, load_sem, pair_s, pair_r, s1, r1, s2, r2, s3, r3):
    count = n_down + n_up
    per_row = down_ref.shape[4] // width
    me = lax.axis_index('data')
    c, x, y, z = coords(me)
    partner = me + 1 - 2 * c
    everyone = [partner]
    for k in range(3):
        pos, stride = axis_of(k, x, y, z)
        everyone += [me + ((pos + d) % 4 - pos) * stride for d in range(1, 4)]
    enter(everyone)

    def axes(u):
        return [axis_of((u + n) % 3, x, y, z) for n in range(3)]

    def remote(a, b, s, r, peer):
        return pltpu.make_async_remote_copy(
            src_ref=a, dst_ref=b, send_sem=s, recv_sem=r, device_id=(peer,), device_id_type=MESH)

    def load_down(u):
        cols = pl.ds(pl.multiple_of((u % per_row) * width, width), width)
        return pltpu.make_async_copy(down_ref.at[:, :, u // per_row, :, cols], src.at[u % 3], load_sem.at[u % 3])

    def load_up(u):
        cols = pl.ds(pl.multiple_of((u - n_down) * width, width), width)
        return pltpu.make_async_copy(up_ref.at[:, :, :, cols], src.at[u % 3], load_sem.at[u % 3])

    def start_load(u):
        @pl.when(u < n_down)
        def _():
            load_down(u).start()

        @pl.when(u >= n_down)
        def _():
            load_up(u).start()

    def pair_copy(u):
        return remote(src.at[u % 3, :, 1 - c], pair_in.at[u], pair_s.at[u], pair_r.at[u], partner)

    def first_copies(u):
        pos, stride = axes(u)[0]
        right = me + ((pos + 1) % 4 - pos) * stride
        left = me + ((pos + 3) % 4 - pos) * stride
        at_r, at_l, at_o = 16 * ((pos + 1) % 4), 16 * ((pos + 3) % 4), 16 * ((pos + 2) % 4)
        buf = work.at[u % 5]
        ends = [
            (at_o, opp_r.at[u], right),
            (at_o + 8, opp_l.at[u], left),
            (at_r + 8, from_l.at[u, pl.ds(8, 8)], right),
            (at_l, from_r.at[u, pl.ds(0, 8)], left),
            (at_r, from_l.at[u, pl.ds(0, 8)], right),
            (at_l + 8, from_r.at[u, pl.ds(8, 8)], left),
        ]
        return [remote(buf.at[pl.ds(at, 8)], dst, s1.at[u, n], r1.at[u, n], peer) for n, (at, dst, peer) in enumerate(ends)]

    def second_copies(u):
        pos, stride = axes(u)[1]
        return [remote(mid.at[u % 3, pl.ds(4 * ((pos + d) % 4), 4)], mid_in.at[u, d - 1], s2.at[u, d - 1], r2.at[u, d - 1],
                       me + ((pos + d) % 4 - pos) * stride) for d in range(1, 4)]

    def third_copies(u):
        pos, stride = axes(u)[2]
        return [remote(low.at[u % 3, (pos + d) % 4], low_in.at[u, d - 1], s3.at[u, d - 1], r3.at[u, d - 1],
                       me + ((pos + d) % 4 - pos) * stride) for d in range(1, 4)]

    def within(u):
        return jnp.logical_and(u >= 0, u < count)

    start_load(0)

    def body(t, _):
        @pl.when(t + 1 < count)
        def _():
            start_load(t + 1)

        @pl.when(t < count)
        def _():
            pltpu.make_async_copy(up_ref.at[:, :, :, pl.ds(0, width)], src.at[t % 3], load_sem.at[t % 3]).wait()
            pair_copy(t).start()

        ub = t - 1

        @pl.when(within(ub))
        def _():
            copy = pair_copy(ub)
            copy.wait_recv()
            (_, st1), (_, st2), (_, st3) = axes(ub)

            def add(b, _):
                at = (b // 4) * (st1 // 2) + (b % 4) * (st2 // 2)
                for n in range(4):
                    here = at + n * (st3 // 2)
                    work[ub % 5, 4 * b + n] = src[ub % 3, here, c] + pair_in[ub, here]
                return 0

            lax.fori_loop(0, 16, add, 0)
            copy.wait_send()
            for copy in first_copies(ub)[:4]:
                copy.start()

        uc = t - 3

        @pl.when(within(uc))
        def _():
            copies = first_copies(uc)
            (pos, _), _, _ = axes(uc)
            at_r, at_l = 16 * ((pos + 1) % 4), 16 * ((pos + 3) % 4)
            copies[0].wait_recv()
            work[uc % 5, pl.ds(at_r, 8)] += opp_r[uc]
            copies[4].start()
            copies[1].wait_recv()
            work[uc % 5, pl.ds(at_l + 8, 8)] += opp_l[uc]
            copies[5].start()

        ud = t - 5

        @pl.when(within(ud))
        def _():
            copies = first_copies(ud)
            for copy in copies[2:]:
                copy.wait_recv()
            (pos, _), _, _ = axes(ud)
            for n in range(0, 16, 4):
                mid[ud % 3, pl.ds(n, 4)] = (work[ud % 5, pl.ds(16 * pos + n, 4)] + from_l[ud, pl.ds(n, 4)]) + from_r[ud, pl.ds(n, 4)]
            for copy in second_copies(ud):
                copy.start()
            for copy in copies:
                copy.wait_send()

        ue = t - 7

        @pl.when(within(ue))
        def _():
            copies = second_copies(ue)
            for copy in copies:
                copy.wait_recv()
            _, (pos, _), _ = axes(ue)
            low[ue % 3] = (mid[ue % 3, pl.ds(4 * pos, 4)] + mid_in[ue, 0]) + (mid_in[ue, 1] + mid_in[ue, 2])
            for copy in third_copies(ue):
                copy.start()
            for copy in copies:
                copy.wait_send()

        uf = t - 9

        @pl.when(within(uf))
        def _():
            copies = third_copies(uf)
            for copy in copies:
                copy.wait_recv()
            _, _, (pos, _) = axes(uf)
            total = (low[uf % 3, pos] + low_in[uf, 0]) + (low_in[uf, 1] + low_in[uf, 2])

            @pl.when(uf < n_down)
            def _():
                out_down[uf // per_row, :, pl.ds(pl.multiple_of((uf % per_row) * width, width), width)] = total

            @pl.when(uf >= n_down)
            def _():
                out_up[:, pl.ds(pl.multiple_of((uf - n_down) * width, width), width)] = total

            for copy in copies:
                copy.wait_send()

        return 0

    lax.fori_loop(0, count + 9, body, 0)


def scatter_grads(grad_down, grad_up, width):
    hidden, model = grad_down.shape
    tiles = hidden // 128 // ROWS
    n_down = tiles * (model // width)
    n_up = hidden // width
    count = n_down + n_up
    f32 = jnp.float32
    block = (ROWS, width)
    out_down, out_up = pl.pallas_call(
        functools.partial(scatter_kernel, n_down, n_up, width),
        out_shape=(jax.ShapeDtypeStruct((tiles, ROWS, model), f32), jax.ShapeDtypeStruct((ROWS, hidden), f32)),
        in_specs=[pl.BlockSpec(memory_space=pl.ANY)] * 2,
        out_specs=(pl.BlockSpec(memory_space=pltpu.VMEM), pl.BlockSpec(memory_space=pltpu.VMEM)),
        scratch_shapes=[
            pltpu.VMEM((3, 64, 2) + block, f32),
            pltpu.VMEM((count, 64) + block, f32),
            pltpu.VMEM((5, 64) + block, f32),
            pltpu.VMEM((count, 8) + block, f32),
            pltpu.VMEM((count, 8) + block, f32),
            pltpu.VMEM((count, 16) + block, f32),
            pltpu.VMEM((count, 16) + block, f32),
            pltpu.VMEM((3, 16) + block, f32),
            pltpu.VMEM((count, 3, 4) + block, f32),
            pltpu.VMEM((3, 4) + block, f32),
            pltpu.VMEM((count, 3) + block, f32),
            pltpu.SemaphoreType.DMA((3,)),
            pltpu.SemaphoreType.DMA((count,)),
            pltpu.SemaphoreType.DMA((count,)),
            pltpu.SemaphoreType.DMA((count, 6)),
            pltpu.SemaphoreType.DMA((count, 6)),
            pltpu.SemaphoreType.DMA((count, 3)),
            pltpu.SemaphoreType.DMA((count, 3)),
            pltpu.SemaphoreType.DMA((count, 3)),
            pltpu.SemaphoreType.DMA((count, 3)),
        ],
        compiler_params=pltpu.CompilerParams(collective_id=1, has_side_effects=True, vmem_limit_bytes=VMEM_BYTES),
    )(grad_down.reshape(64, 2, tiles, ROWS, model), grad_up.reshape(64, 2, ROWS, hidden))
    return out_down.reshape(hidden // 128, model), out_up


def solution(mesh):
    group_size = mesh.shape['data']

    def local_step(tok_rows, w_up, w_down, heads, label_rows):
        total_rows = tok_rows.shape[0] * group_size
        num_classes = heads.shape[2]
        pre_act = jnp.dot(tok_rows, w_up, preferred_element_type=jnp.float32).astype(jnp.bfloat16)
        hidden = jax.nn.gelu(pre_act.astype(jnp.float32)).astype(jnp.bfloat16)
        trunk_out = tok_rows.astype(jnp.float32) + jnp.dot(hidden, w_down, preferred_element_type=jnp.float32)
        logits = jnp.einsum('bd,tdc->tbc', trunk_out.astype(jnp.bfloat16), heads, preferred_element_type=jnp.float32)
        onehot = (label_rows[:, :, None] == jnp.arange(num_classes)[None, None, :]).astype(jnp.float32)
        task_resid = (jax.nn.softmax(logits, axis=-1) - onehot) / total_rows
        heads_f32 = heads.astype(jnp.float32)
        head_gram = jnp.einsum('tdc,sde->tcse', heads_f32, heads_f32, precision=EXACT_PREC)
        res_outer = jnp.einsum('tbc,sbe->tcse', task_resid, task_resid, precision=EXACT_PREC)
        part_gram = jnp.sum(res_outer * head_gram, axis=(1, 3))
        mix_wts = solve_weights(part_gram)
        d_out = jnp.einsum('tbc,tdc->bd', task_resid * mix_wts[:, None, None], heads_f32, precision=EXACT_PREC).astype(jnp.bfloat16)
        grad_down = lax.dot_general(hidden, d_out, (((0,), (0,)), ((), ())), preferred_element_type=jnp.float32)
        d_hidden = lax.dot_general(d_out, w_down, (((1,), (1,)), ((), ())), preferred_element_type=jnp.float32)
        gelu_vjp = jax.vjp(jax.nn.gelu, pre_act.astype(jnp.float32))[1]
        d_pre = gelu_vjp(d_hidden)[0].astype(jnp.bfloat16)
        tok_cols = lax.optimization_barrier(tok_rows.T)
        grad_up = jnp.dot(tok_cols, d_pre, preferred_element_type=jnp.float32)
        down_shard, up_shard = scatter_grads(grad_down, grad_up, 512)
        return mix_wts, up_shard, down_shard

    return jax.shard_map(local_step, mesh=mesh, in_specs=(P('data', None), P(), P(), P(), P(None, 'data')), out_specs=(P(), P('data', None), P('data', None)), check_vma=False)
```

```python
import functools

import jax
import jax.numpy as jnp
from jax import lax
from jax.experimental import pallas as pl
from jax.experimental.pallas import tpu as pltpu
from jax.sharding import PartitionSpec as P

SOLVER_STEPS = 20
EXACT_PREC = lax.Precision.HIGHEST
MESH = pl.DeviceIdType.MESH
VMEM_BYTES = 67_043_328
ROWS = 8


def coords(me):
    return me % 2, (me // 2) % 4, (me // 8) % 4, me // 32


def axis_of(k, x, y, z):
    wz = (k - 1) * (k - 2) // 2
    wy = k * (2 - k)
    wx = k * (k - 1) // 2
    return z * wz + y * wy + x * wx, 32 * wz + 8 * wy + 2 * wx


def enter(peers):
    barrier = pltpu.get_barrier_semaphore()
    for peer in peers:
        pl.semaphore_signal(barrier, inc=1, device_id=(peer,), device_id_type=MESH)
    pl.semaphore_wait(barrier, len(peers))


def gram_kernel(gram_ref, tok_ref, wts_ref, cols_ref, stage0, stage1, stage2, tot0, tot1, send_sem, recv_sem):
    me = lax.axis_index('data')
    c, x, y, z = coords(me)
    low = me % 8
    group0 = [me - low + (low + d) % 8 for d in range(1, 8)]
    group1 = [me + ((y + d) % 4 - y) * 8 for d in range(1, 4)]
    group2 = [me + ((z + d) % 4 - z) * 32 for d in range(1, 4)]
    enter(group0 + group1 + group2)

    def exchange(src, slots, slot, group, first, beside=None):
        copies = []
        for n, peer in enumerate(group):
            copy = pltpu.make_async_remote_copy(
                src_ref=src,
                dst_ref=slots.at[slot],
                send_sem=send_sem.at[first + n],
                recv_sem=recv_sem.at[first + n],
                device_id=(peer,),
                device_id_type=MESH,
            )
            copy.start()
            copies.append(copy)
        slots[slot] = src[...]
        if beside is not None:
            beside()
        for copy in copies:
            copy.wait()

    def transpose():
        cols_ref[...] = tok_ref[...].T

    exchange(gram_ref, stage0, low, group0, 0, transpose)
    tot0[...] = sum(stage0[n] for n in range(1, 8)) + stage0[0]
    exchange(tot0, stage1, y, group1, 7)
    tot1[...] = (stage1[0] + stage1[1]) + (stage1[2] + stage1[3])
    exchange(tot1, stage2, z, group2, 10)
    full = (stage2[0] + stage2[1]) + (stage2[2] + stage2[3])
    gram, gram_t = full[0], full[1]
    row = lax.broadcasted_iota(jnp.int32, gram.shape, 0)
    lane = lax.broadcasted_iota(jnp.int32, gram.shape, 1)
    trace = jnp.sum(jnp.where(row == lane, gram, 0.0), axis=(0, 1), keepdims=True)
    scale = jnp.broadcast_to(trace / 4, gram.shape)
    by_lane = jnp.where(lane < 4, 0.25, 0.0)
    by_row = jnp.where(row < 4, 0.25, 0.0)
    for _ in range(SOLVER_STEPS):
        down_row = jnp.sum(gram * by_lane, axis=1, keepdims=True)
        down_lane = jnp.sum(gram_t * by_row, axis=0, keepdims=True)
        by_row = by_row * jnp.exp(-down_row / scale)
        by_lane = by_lane * jnp.exp(-down_lane / scale)
        by_row = by_row / jnp.sum(by_row, axis=0, keepdims=True)
        by_lane = by_lane / jnp.sum(by_lane, axis=1, keepdims=True)
    wts_ref[...] = by_lane


def solve_weights(part_gram, tok_rows):
    pads = ((0, 0), (0, 4), (0, 124))
    both = jnp.pad(jnp.stack([part_gram, part_gram.T]), pads)
    vmem = pl.BlockSpec(memory_space=pltpu.VMEM)
    wts, tok_cols = pl.pallas_call(
        gram_kernel,
        out_shape=(jax.ShapeDtypeStruct((8, 128), jnp.float32), jax.ShapeDtypeStruct(tok_rows.shape[::-1], tok_rows.dtype)),
        in_specs=[vmem, vmem],
        out_specs=(vmem, vmem),
        scratch_shapes=[
            pltpu.VMEM((8, 2, 8, 128), jnp.float32),
            pltpu.VMEM((4, 2, 8, 128), jnp.float32),
            pltpu.VMEM((4, 2, 8, 128), jnp.float32),
            pltpu.VMEM((2, 8, 128), jnp.float32),
            pltpu.VMEM((2, 8, 128), jnp.float32),
            pltpu.SemaphoreType.DMA((13,)),
            pltpu.SemaphoreType.DMA((13,)),
        ],
        compiler_params=pltpu.CompilerParams(collective_id=0, has_side_effects=True),
    )(both, tok_rows)
    return wts[0, :4], tok_cols


TOK = 512
WIDTH = 512
GELU_C = 0.7978845608028654
GELU_K = 0.044715


def backward_kernel(n_up, n_down, pre_ref, dz_ref, wd_ref, xt_ref, out_up, out_down,
                    xt, dz, p_t, pre, wd, d_pre, dh_a, dh_b, p_buf,
                    src, pair_in, work, opp_r, opp_l, from_l, from_r, mid, mid_in, low, low_in,
                    xt_sem, dz_sem, pre_sem, wd_sem, pair_s, pair_r, s1, r1, s2, r2, s3, r3):
    count = n_up + n_down
    me = lax.axis_index('data')
    c, x, y, z = coords(me)
    partner = me + 1 - 2 * c
    everyone = [partner]
    for k in range(3):
        pos, stride = axis_of(k, x, y, z)
        everyone += [me + ((pos + d) % 4 - pos) * stride for d in range(1, 4)]

    tiles = dz.shape[0] // TOK
    n_tiles = n_up * tiles

    def load_pre(g):
        rows = pl.ds(pl.multiple_of((g % tiles) * TOK, TOK), TOK)
        cols = pl.ds(pl.multiple_of((g // tiles) * WIDTH, WIDTH), WIDTH)
        return pltpu.make_async_copy(pre_ref.at[rows, cols], pre.at[g % 3], pre_sem.at[g % 3])

    def load_wd(j):
        rows = pl.ds(pl.multiple_of(j * WIDTH, WIDTH), WIDTH)
        return pltpu.make_async_copy(wd_ref.at[rows], wd.at[j % 2], wd_sem.at[j % 2])

    load_dz = pltpu.make_async_copy(dz_ref, dz, dz_sem)
    load_xt = pltpu.make_async_copy(xt_ref, xt, xt_sem)
    load_wd(0).start()
    load_dz.start()
    load_pre(0).start()
    load_pre(1).start()
    load_wd(1).start()
    load_xt.start()
    enter(everyone)

    def axes(u):
        return [axis_of((u + n) % 3, x, y, z) for n in range(3)]

    def remote(a, b, s, r, peer):
        return pltpu.make_async_remote_copy(
            src_ref=a, dst_ref=b, send_sem=s, recv_sem=r, device_id=(peer,), device_id_type=MESH)

    def pair_copy(u):
        return remote(src.at[u % 2, :, 1 - c], pair_in.at[u % 4], pair_s.at[u % 4], pair_r.at[u % 4], partner)

    def first_copies(u):
        pos, stride = axes(u)[0]
        right = me + ((pos + 1) % 4 - pos) * stride
        left = me + ((pos + 3) % 4 - pos) * stride
        at_r, at_l, at_o = 16 * ((pos + 1) % 4), 16 * ((pos + 3) % 4), 16 * ((pos + 2) % 4)
        buf = work.at[u % 4]
        ends = [
            (at_o, opp_r.at[u], right),
            (at_o + 8, opp_l.at[u], left),
            (at_r + 8, from_l.at[u, pl.ds(8, 8)], right),
            (at_l, from_r.at[u, pl.ds(0, 8)], left),
            (at_r, from_l.at[u, pl.ds(0, 8)], right),
            (at_l + 8, from_r.at[u, pl.ds(8, 8)], left),
        ]
        return [remote(buf.at[pl.ds(at, 8)], dst, s1.at[u, n], r1.at[u, n], peer) for n, (at, dst, peer) in enumerate(ends)]

    def second_copies(u):
        pos, stride = axes(u)[1]
        return [remote(mid.at[u % 3, pl.ds(4 * ((pos + d) % 4), 4)], mid_in.at[u, d - 1], s2.at[u, d - 1], r2.at[u, d - 1],
                       me + ((pos + d) % 4 - pos) * stride) for d in range(1, 4)]

    def third_copies(u):
        pos, stride = axes(u)[2]
        return [remote(low.at[u % 3, (pos + d) % 4], low_in.at[u, d - 1], s3.at[u, d - 1], r3.at[u, d - 1],
                       me + ((pos + d) % 4 - pos) * stride) for d in range(1, 4)]

    def within(u):
        return jnp.logical_and(u >= 0, u < count)

    def dh_dot(g, out):
        rows = pl.ds(pl.multiple_of((g % tiles) * TOK, TOK), TOK)
        out[...] = lax.dot_general(dz[rows], wd[(g // tiles) % 2], (((1,), (1,)), ((), ())), preferred_element_type=jnp.float32)

    def act_tile(g, dh):
        slot = g % 3
        at = pl.multiple_of((g % tiles) * TOK, TOK)
        for r in range(0, TOK, 32):
            v = pre[slot, r:r + 32].astype(jnp.float32)
            sq = v * v
            th = jnp.tanh(v * (GELU_C + (GELU_C * GELU_K) * sq))
            cdf = 0.5 + 0.5 * th
            p_buf[r:r + 32] = (v * cdf).astype(jnp.bfloat16)
            slope = cdf + (0.5 * v) * (1.0 - th * th) * (GELU_C + (3 * GELU_C * GELU_K) * sq)
            d_pre[pl.ds(at + r, 32)] = (dh[r:r + 32] * slope).astype(jnp.bfloat16)
        flipped = p_buf[...].T
        p_t[pl.ds(pl.multiple_of((g // tiles) * (WIDTH // 32), WIDTH // 32), WIDTH // 32), :, :, pl.ds(at, TOK)] = flipped.reshape(WIDTH // 32, 2, 16, TOK)

    def produce_up(t):
        @pl.when(t == 0)
        def _():
            load_wd(0).wait()
            load_dz.wait()
            dh_dot(0, dh_a)

        @pl.when(t + 1 < n_up)
        def _():
            load_wd(t + 1).wait()

        def step(i, _):
            for half, (now, then) in enumerate(((dh_a, dh_b), (dh_b, dh_a))):
                g = t * tiles + 2 * i + half

                @pl.when(g + 2 < n_tiles)
                def _():
                    load_pre(g + 2).start()

                load_pre(g).wait()
                dh_dot(g + 1, then)
                act_tile(g, now)
            return 0

        lax.fori_loop(0, tiles // 2, step, 0)

        @pl.when(t + 2 < n_up)
        def _():
            load_wd(t + 2).start()

        @pl.when(t == 0)
        def _():
            load_xt.wait()

        prod = jnp.dot(xt[...], d_pre[...], preferred_element_type=jnp.float32)
        src[t % 2] = prod.reshape(64, 2, ROWS, WIDTH)

    def produce_down(t):
        u = t - n_up
        half = u % 2
        cols = pl.ds(pl.multiple_of((u // 2) * 256, 256), 256)
        for m in range(2):
            rows = p_t[pl.ds(64 * m, 64), half].reshape(1024, p_t.shape[3])
            prod = jnp.dot(rows, dz[:, cols], preferred_element_type=jnp.float32)
            prod = prod.reshape(32, 2, 2, ROWS, 256)
            src[t % 2, pl.ds(32 * m, 32), :, :, 0:256] = prod[:, :, 0]
            src[t % 2, pl.ds(32 * m, 32), :, :, 256:512] = prod[:, :, 1]

    def body(t, _):
        @pl.when(t < n_up)
        def _():
            produce_up(t)

        @pl.when(jnp.logical_and(t >= n_up, t < count))
        def _():
            produce_down(t)

        @pl.when(t < count)
        def _():
            pair_copy(t).start()

        uc = t - 3

        @pl.when(within(uc))
        def _():
            copies = first_copies(uc)
            (pos, _), _, _ = axes(uc)
            at_r, at_l = 16 * ((pos + 1) % 4), 16 * ((pos + 3) % 4)
            copies[0].wait_recv()
            work[uc % 4, pl.ds(at_r, 8)] += opp_r[uc]
            copies[4].start()
            copies[1].wait_recv()
            work[uc % 4, pl.ds(at_l + 8, 8)] += opp_l[uc]
            copies[5].start()

        ud = t - 5

        @pl.when(within(ud))
        def _():
            copies = first_copies(ud)
            for copy in copies[2:]:
                copy.wait_recv()
            (pos, _), _, _ = axes(ud)
            for n in range(0, 16, 4):
                mid[ud % 3, pl.ds(n, 4)] = (work[ud % 4, pl.ds(16 * pos + n, 4)] + from_l[ud, pl.ds(n, 4)]) + from_r[ud, pl.ds(n, 4)]
            for copy in second_copies(ud):
                copy.start()
            for copy in copies:
                copy.wait_send()

        ub = t - 1

        @pl.when(within(ub))
        def _():
            copy = pair_copy(ub)
            copy.wait_recv()
            (_, st1), (_, st2), (_, st3) = axes(ub)

            def add(b, _):
                at = (b // 4) * (st1 // 2) + (b % 4) * (st2 // 2)
                for n in range(4):
                    here = at + n * (st3 // 2)
                    work[ub % 4, 4 * b + n] = src[ub % 2, here, c] + pair_in[ub % 4, here]
                return 0

            lax.fori_loop(0, 16, add, 0)
            copy.wait_send()
            for copy in first_copies(ub)[:4]:
                copy.start()

        ue = t - 7

        @pl.when(within(ue))
        def _():
            copies = second_copies(ue)
            for copy in copies:
                copy.wait_recv()
            _, (pos, _), _ = axes(ue)
            low[ue % 3] = (mid[ue % 3, pl.ds(4 * pos, 4)] + mid_in[ue, 0]) + (mid_in[ue, 1] + mid_in[ue, 2])
            for copy in third_copies(ue):
                copy.start()
            for copy in copies:
                copy.wait_send()

        uf = t - 9

        @pl.when(within(uf))
        def _():
            copies = third_copies(uf)
            for copy in copies:
                copy.wait_recv()
            _, _, (pos, _) = axes(uf)
            total = (low[uf % 3, pos] + low_in[uf, 0]) + (low_in[uf, 1] + low_in[uf, 2])

            @pl.when(uf < n_up)
            def _():
                out_up[:, pl.ds(pl.multiple_of(uf * WIDTH, WIDTH), WIDTH)] = total

            @pl.when(uf >= n_up)
            def _():
                tile = uf - n_up
                cols = pl.ds(pl.multiple_of((tile // 2) * 256, 256), 256)
                out_down[2 * (tile % 2), :, cols] = total[:, 0:256]
                out_down[2 * (tile % 2) + 1, :, cols] = total[:, 256:512]

            for copy in copies:
                copy.wait_send()

        return 0

    lax.fori_loop(0, count + 9, body, 0)


def backward(pre_act, d_out, w_down, tok_cols):
    tokens, hidden = pre_act.shape
    model = d_out.shape[1]
    n_up, n_down = hidden // WIDTH, 2 * (model // 256)
    count = n_up + n_down
    f32, bf16 = jnp.float32, jnp.bfloat16
    block = (ROWS, WIDTH)
    dma = pltpu.SemaphoreType.DMA
    out_up, out_down = pl.pallas_call(
        functools.partial(backward_kernel, n_up, n_down),
        out_shape=(jax.ShapeDtypeStruct((ROWS, hidden), f32), jax.ShapeDtypeStruct((4, ROWS, model), f32)),
        in_specs=[pl.BlockSpec(memory_space=pl.ANY)] * 4,
        out_specs=(pl.BlockSpec(memory_space=pltpu.VMEM), pl.BlockSpec(memory_space=pltpu.VMEM)),
        scratch_shapes=[
            pltpu.VMEM((model, tokens), bf16),
            pltpu.VMEM((tokens, model), bf16),
            pltpu.VMEM((hidden // 32, 2, 16, tokens), bf16),
            pltpu.VMEM((3, TOK, WIDTH), bf16),
            pltpu.VMEM((2, WIDTH, model), bf16),
            pltpu.VMEM((tokens, WIDTH), bf16),
            pltpu.VMEM((TOK, WIDTH), f32),
            pltpu.VMEM((TOK, WIDTH), f32),
            pltpu.VMEM((TOK, WIDTH), bf16),
            pltpu.VMEM((2, 64, 2) + block, f32),
            pltpu.VMEM((4, 64) + block, f32),
            pltpu.VMEM((4, 64) + block, f32),
            pltpu.VMEM((count, 8) + block, f32),
            pltpu.VMEM((count, 8) + block, f32),
            pltpu.VMEM((count, 16) + block, f32),
            pltpu.VMEM((count, 16) + block, f32),
            pltpu.VMEM((3, 16) + block, f32),
            pltpu.VMEM((count, 3, 4) + block, f32),
            pltpu.VMEM((3, 4) + block, f32),
            pltpu.VMEM((count, 3) + block, f32),
            dma, dma, dma((3,)), dma((2,)), dma((4,)), dma((4,)),
            dma((count, 6)), dma((count, 6)), dma((count, 3)), dma((count, 3)), dma((count, 3)), dma((count, 3)),
        ],
        compiler_params=pltpu.CompilerParams(collective_id=1, has_side_effects=True, vmem_limit_bytes=VMEM_BYTES),
    )(pre_act, d_out, w_down, tok_cols)
    return out_up, out_down.reshape(hidden // 128, model)


def solution(mesh):
    group_size = mesh.shape['data']

    def local_step(tok_rows, w_up, w_down, heads, label_rows):
        total_rows = tok_rows.shape[0] * group_size
        num_classes = heads.shape[2]
        pre_act = jnp.dot(tok_rows, w_up, preferred_element_type=jnp.float32).astype(jnp.bfloat16)
        hidden = jax.nn.gelu(pre_act.astype(jnp.float32)).astype(jnp.bfloat16)
        trunk_out = tok_rows.astype(jnp.float32) + jnp.dot(hidden, w_down, preferred_element_type=jnp.float32)
        logits = jnp.einsum('bd,tdc->tbc', trunk_out.astype(jnp.bfloat16), heads, preferred_element_type=jnp.float32)
        onehot = (label_rows[:, :, None] == jnp.arange(num_classes)[None, None, :]).astype(jnp.float32)
        task_resid = (jax.nn.softmax(logits, axis=-1) - onehot) / total_rows
        heads_f32 = heads.astype(jnp.float32)
        head_gram = jnp.einsum('tdc,sde->tcse', heads_f32, heads_f32, precision=EXACT_PREC)
        res_outer = jnp.einsum('tbc,sbe->tcse', task_resid, task_resid, precision=EXACT_PREC)
        part_gram = jnp.sum(res_outer * head_gram, axis=(1, 3))
        mix_wts, tok_cols = solve_weights(part_gram, tok_rows)
        d_out = jnp.einsum('tbc,tdc->bd', task_resid * mix_wts[:, None, None], heads_f32, precision=EXACT_PREC).astype(jnp.bfloat16)
        up_shard, down_shard = backward(pre_act, d_out, w_down, tok_cols)
        return mix_wts, up_shard, down_shard

    return jax.shard_map(local_step, mesh=mesh, in_specs=(P('data', None), P(), P(), P(), P(None, 'data')), out_specs=(P(), P('data', None), P('data', None)), check_vma=False)
```

```python
import functools

import jax
import jax.numpy as jnp
from jax import lax
from jax.experimental import pallas as pl
from jax.experimental.pallas import tpu as pltpu
from jax.sharding import PartitionSpec as P

SOLVER_STEPS = 20
MESH = pl.DeviceIdType.MESH
VMEM_BYTES = 67_043_328
ROWS = 8


def coords(me):
    return me % 2, (me // 2) % 4, (me // 8) % 4, me // 32


def axis_of(k, x, y, z):
    wz = (k - 1) * (k - 2) // 2
    wy = k * (2 - k)
    wx = k * (k - 1) // 2
    return z * wz + y * wy + x * wx, 32 * wz + 8 * wy + 2 * wx


def enter(peers):
    barrier = pltpu.get_barrier_semaphore()
    for peer in peers:
        pl.semaphore_signal(barrier, inc=1, device_id=(peer,), device_id_type=MESH)
    pl.semaphore_wait(barrier, len(peers))


def three_terms(v):
    hi = v.astype(jnp.bfloat16)
    rest = v - hi.astype(jnp.float32)
    mid = rest.astype(jnp.bfloat16)
    low = (rest - mid.astype(jnp.float32)).astype(jnp.bfloat16)
    return hi, mid, low


def nt_dot(a, b):
    return lax.dot_general(a, b, (((1,), (1,)), ((), ())), preferred_element_type=jnp.float32)


def gram_kernel(total_rows, logit_ref, label_ref, heads_ref, wts_ref, dz_ref, gram_ref, flip, resid, terms, heads3, wide,
                stage0, stage1, stage2, tot0, tot1, send_sem, recv_sem):
    me = lax.axis_index('data')
    c, x, y, z = coords(me)
    low = me % 8
    group0 = [me - low + (low + d) % 8 for d in range(1, 8)]
    group1 = [me + ((y + d) % 4 - y) * 8 for d in range(1, 4)]
    group2 = [me + ((z + d) % 4 - z) * 32 for d in range(1, 4)]
    barrier = pltpu.get_barrier_semaphore()
    for peer in group0 + group1 + group2:
        pl.semaphore_signal(barrier, inc=1, device_id=(peer,), device_id_type=MESH)

    tokens = logit_ref.shape[1]
    logits = [logit_ref[8 * n:8 * n + 4] for n in range(3)]
    top = jnp.maximum(jnp.maximum(logits[0], logits[1]), logits[2])
    exps = [jnp.exp(v - top) for v in logits]
    total = (exps[0] + exps[1]) + exps[2]
    resid[...] = jnp.zeros_like(resid)
    labels = label_ref[...]
    for n in range(3):
        hit = (labels == n).astype(jnp.float32)
        resid[8 * n:8 * n + 4] = (exps[n] / total - hit) / total_rows
    heads = stack_heads(heads_ref, wide)
    for n, part in enumerate(three_terms(resid[...])):
        terms[32 * n:32 * n + 32] = part
        heads3[32 * n:32 * n + 32] = heads
    with_hi = nt_dot(terms[...], terms[0:32])
    with_mid = nt_dot(terms[0:64], terms[32:64])
    outer = (with_hi[0:32] + with_mid[0:32] + with_hi[32:64]) + (nt_dot(terms[0:32], terms[64:96]) + with_hi[64:96] + with_mid[32:64])
    outer = outer * nt_dot(heads, heads)
    flip[...] = jnp.zeros_like(flip)
    flip[0:8, 0:32] = outer[0:8] + outer[8:16] + outer[16:24]
    turned = flip[...].T
    gram_t = turned[0:8] + turned[8:16] + turned[16:24]
    flip[0:8] = gram_t
    turned = flip[...].T
    gram_ref[0] = turned[0:8]
    gram_ref[1] = gram_t
    pl.semaphore_wait(barrier, 13)

    def exchange(src, slots, slot, group, first):
        copies = []
        for n, peer in enumerate(group):
            copy = pltpu.make_async_remote_copy(
                src_ref=src,
                dst_ref=slots.at[slot],
                send_sem=send_sem.at[first + n],
                recv_sem=recv_sem.at[first + n],
                device_id=(peer,),
                device_id_type=MESH,
            )
            copy.start()
            copies.append(copy)
        slots[slot] = src[...]
        for copy in copies:
            copy.wait()

    exchange(gram_ref, stage0, low, group0, 0)
    tot0[...] = sum(stage0[n] for n in range(1, 8)) + stage0[0]
    exchange(tot0, stage1, y, group1, 7)
    tot1[...] = (stage1[0] + stage1[1]) + (stage1[2] + stage1[3])
    exchange(tot1, stage2, z, group2, 10)
    full = (stage2[0] + stage2[1]) + (stage2[2] + stage2[3])
    gram, gram_t = full[0], full[1]
    row = lax.broadcasted_iota(jnp.int32, gram.shape, 0)
    lane = lax.broadcasted_iota(jnp.int32, gram.shape, 1)
    trace = jnp.sum(jnp.where(row == lane, gram, 0.0), axis=(0, 1), keepdims=True)
    scale = jnp.broadcast_to(trace / 4, gram.shape)
    gram, gram_t = gram / scale, gram_t / scale
    by_lane = jnp.where(lane < 4, 0.25, 0.0)
    by_row = jnp.where(row < 4, 0.25, 0.0)
    for _ in range(SOLVER_STEPS):
        down_row = jnp.sum(gram * by_lane, axis=1, keepdims=True)
        down_lane = jnp.sum(gram_t * by_row, axis=0, keepdims=True)
        by_row = by_row * jnp.exp(-down_row)
        by_lane = by_lane * jnp.exp(-down_lane)
        by_row = by_row / jnp.sum(by_row, axis=0, keepdims=True)
        by_lane = by_lane / jnp.sum(by_lane, axis=1, keepdims=True)
    wts_ref[...] = by_lane[0:1, 0:4]
    wide = jnp.broadcast_to(by_row[:, 0:1], (8, tokens))
    for n in range(3):
        resid[8 * n:8 * n + 8] = resid[8 * n:8 * n + 8] * wide
    for n, part in enumerate(three_terms(resid[...])):
        terms[32 * n:32 * n + 32] = part

    def rows_out(i, _):
        at = pl.ds(pl.multiple_of(i * 256, 256), 256)
        out = lax.dot_general(terms[:, at], heads3[...], (((0,), (0,)), ((), ())), preferred_element_type=jnp.float32)
        dz_ref[at] = out.astype(jnp.bfloat16)
        return 0

    lax.fori_loop(0, tokens // 256, rows_out, 0)


def solve_weights(logits, labels, heads, total_rows):
    tokens = logits.shape[1]
    model = heads.shape[2]
    f32, bf16 = jnp.float32, jnp.bfloat16
    vmem = pl.BlockSpec(memory_space=pltpu.VMEM)
    wts, d_out = pl.pallas_call(
        functools.partial(gram_kernel, total_rows),
        out_shape=(jax.ShapeDtypeStruct((1, 4), f32), jax.ShapeDtypeStruct((tokens, model), bf16)),
        in_specs=[vmem] * 3,
        out_specs=(vmem, vmem),
        scratch_shapes=[
            pltpu.VMEM((2, 8, 128), f32),
            pltpu.VMEM((128, 128), f32),
            pltpu.VMEM((32, tokens), f32),
            pltpu.VMEM((96, tokens), bf16),
            pltpu.VMEM((96, model), bf16),
            pltpu.VMEM((32, model), f32),
            pltpu.VMEM((8, 2, 8, 128), f32),
            pltpu.VMEM((4, 2, 8, 128), f32),
            pltpu.VMEM((4, 2, 8, 128), f32),
            pltpu.VMEM((2, 8, 128), f32),
            pltpu.VMEM((2, 8, 128), f32),
            pltpu.SemaphoreType.DMA((13,)),
            pltpu.SemaphoreType.DMA((13,)),
        ],
        compiler_params=pltpu.CompilerParams(collective_id=0, has_side_effects=True),
    )(logits, labels, heads)
    return wts[0], d_out


TOK = 512
WIDTH = 512
GELU_C = 0.7978845608028654
GELU_K = 0.044715


def stack_heads(heads_ref, wide):
    wide[...] = jnp.zeros_like(wide)
    for n in range(heads_ref.shape[0]):
        wide[8 * n:8 * n + heads_ref.shape[1]] = heads_ref[n].astype(jnp.float32)
    return wide[...].astype(jnp.bfloat16)


def forward_kernel(tok_ref, wu_ref, wd_ref, heads_ref, slope_ref, pt_ref, xt_ref, logit_ref,
                   tok, wu, wd, act_a, act_b, hid, total, slope, flipped, turned, wide, heads,
                   tok_sem, wu_sem, wd_sem, slope_sem, flip_sem, turn_sem):
    n_tok = tok.shape[0] // TOK
    n_hid = wu.shape[0]
    n_out = wd.shape[0]

    def tok_rows(i):
        return pl.ds(pl.multiple_of(i * TOK, TOK), TOK)

    def load_tok(i):
        return pltpu.make_async_copy(tok_ref.at[tok_rows(i)], tok.at[tok_rows(i)], tok_sem.at[i])

    def load_wu(j):
        cols = pl.ds(pl.multiple_of(j * WIDTH, WIDTH), WIDTH)
        return pltpu.make_async_copy(wu_ref.at[:, cols], wu.at[j], wu_sem.at[j])

    def load_wd(n):
        cols = pl.ds(pl.multiple_of(n * 256, 256), 256)
        return pltpu.make_async_copy(wd_ref.at[:, cols], wd.at[n], wd_sem.at[n])

    def stores(i, j, b):
        cols = pl.ds(pl.multiple_of(j * WIDTH, WIDTH), WIDTH)
        group = pl.ds(j * (WIDTH // 32), WIDTH // 32)
        feats = pl.ds(pl.multiple_of(j * 128, 128), 128)
        return [
            pltpu.make_async_copy(slope.at[b], slope_ref.at[tok_rows(i), cols], slope_sem.at[b]),
            pltpu.make_async_copy(flipped.at[b], pt_ref.at[group, :, :, tok_rows(i)], flip_sem.at[b]),
            pltpu.make_async_copy(turned.at[b], xt_ref.at[feats, tok_rows(i)], turn_sem.at[b]),
        ]

    load_tok(0).start()
    for n in range(n_hid):
        load_wu(n).start()
    load_tok(1).start()
    for n in range(n_out):
        load_wd(n).start()
    for n in range(2, n_tok):
        load_tok(n).start()
    heads[...] = stack_heads(heads_ref, wide)

    def act_dot(i, j, out):
        out[...] = jnp.dot(tok[tok_rows(i)], wu[j], preferred_element_type=jnp.float32).astype(jnp.bfloat16)

    def finish(i):
        def block(n, _):
            cols = pl.ds(pl.multiple_of(n * 256, 256), 256)
            total[:, cols] = jnp.dot(hid[...], wd[n], preferred_element_type=jnp.float32)
            return 0

        lax.fori_loop(0, n_out, block, 0)
        low = (total[...] + tok[tok_rows(i)].astype(jnp.float32)).astype(jnp.bfloat16)
        logit_ref[:, tok_rows(i)] = nt_dot(heads[...], low)

    def half_step(i, j, b, act, act_next, first):
        at_j = pl.ds(pl.multiple_of(j * WIDTH, WIDTH), WIDTH)
        if first:
            @pl.when(j + 1 < n_hid)
            def _():
                load_wu(j + 1).wait()

            @pl.when(j >= 2)
            def _():
                for copy in stores(i, j, b):
                    copy.wait()
        else:
            for copy in stores(i, j, b):
                copy.wait()

        if b == 1:
            @pl.when(jnp.logical_and(j == n_hid - 1, i + 1 < n_tok))
            def _():
                load_tok(i + 1).wait()

        step = i * n_hid + j + 1
        act_dot((step // n_hid) % n_tok, step % n_hid, act_next)
        for r in range(0, TOK, 32):
            v = act[r:r + 32].astype(jnp.float32)
            cub = (v * v) * (GELU_C * GELU_K)
            inner = cub + GELU_C
            th = jnp.tanh(v * inner)
            cdf = 0.5 * th + 0.5
            p = v * cdf
            hid[r:r + 32, at_j] = p.astype(jnp.bfloat16)
            slope[b, r:r + 32] = (p * (1.0 - th)) * (inner + (cub + cub)) + cdf
        flipped[b] = hid[:, at_j].T.reshape(WIDTH // 32, 2, 16, TOK)
        feats = pl.ds(pl.multiple_of(j * 128, 128), 128)
        turned[b] = tok[tok_rows(i), feats].T
        for copy in stores(i, j, b):
            copy.start()

    def tile(i, first):
        def pair(k, _):
            half_step(i, 2 * k, 0, act_a, act_b, first)
            half_step(i, 2 * k + 1, 1, act_b, act_a, first)
            return 0

        lax.fori_loop(0, n_hid // 2, pair, 0)

    load_tok(0).wait()
    load_wu(0).wait()
    act_dot(0, 0, act_a)
    tile(0, True)
    for n in range(n_out):
        load_wd(n).wait()
    finish(0)

    def later(i, _):
        tile(i, False)
        finish(i)
        return 0

    lax.fori_loop(1, n_tok, later, 0)
    for b in range(2):
        for copy in stores(n_tok - 1, n_hid - 2 + b, b):
            copy.wait()


def forward(tok_rows, w_up, w_down, heads):
    tokens, model = tok_rows.shape
    hidden = w_up.shape[1]
    n_hid = hidden // WIDTH
    f32, bf16 = jnp.float32, jnp.bfloat16
    dma = pltpu.SemaphoreType.DMA
    hbm, vmem = pl.BlockSpec(memory_space=pl.ANY), pl.BlockSpec(memory_space=pltpu.VMEM)
    return pl.pallas_call(
        forward_kernel,
        out_shape=(
            jax.ShapeDtypeStruct((tokens, hidden), f32),
            jax.ShapeDtypeStruct((hidden // 32, 2, 16, tokens), bf16),
            jax.ShapeDtypeStruct((model, tokens), bf16),
            jax.ShapeDtypeStruct((32, tokens), f32),
        ),
        in_specs=[hbm, hbm, hbm, vmem],
        out_specs=(hbm, hbm, hbm, vmem),
        scratch_shapes=[
            pltpu.VMEM((tokens, model), bf16),
            pltpu.VMEM((n_hid, model, WIDTH), bf16),
            pltpu.VMEM((model // 256, hidden, 256), bf16),
            pltpu.VMEM((TOK, WIDTH), bf16),
            pltpu.VMEM((TOK, WIDTH), bf16),
            pltpu.VMEM((TOK, hidden), bf16),
            pltpu.VMEM((TOK, model), f32),
            pltpu.VMEM((2, TOK, WIDTH), f32),
            pltpu.VMEM((2, WIDTH // 32, 2, 16, TOK), bf16),
            pltpu.VMEM((2, 128, TOK), bf16),
            pltpu.VMEM((32, model), f32),
            pltpu.VMEM((32, model), bf16),
            dma((tokens // TOK,)), dma((n_hid,)), dma((model // 256,)), dma((2,)), dma((2,)), dma((2,)),
        ],
        compiler_params=pltpu.CompilerParams(
            vmem_limit_bytes=VMEM_BYTES),
    )(tok_rows, w_up, w_down, heads)


def backward_kernel(n_up, n_down, slope_ref, dz_ref, wd_ref, xt_ref, pt_ref, out_up, out_down,
                    xt, dz, p_t, slope, wd, d_pre,
                    src, pair_in, work, opp_r, opp_l, from_l, from_r, mid, mid_in, low, low_in,
                    xt_sem, dz_sem, pt_sem, slope_sem, wd_sem, pair_s, pair_r, s1, r1, s2, r2, s3, r3):
    count = n_up + n_down
    me = lax.axis_index('data')
    c, x, y, z = coords(me)
    partner = me + 1 - 2 * c
    everyone = [partner]
    for k in range(3):
        pos, stride = axis_of(k, x, y, z)
        everyone += [me + ((pos + d) % 4 - pos) * stride for d in range(1, 4)]

    tiles = dz.shape[0] // TOK
    n_tiles = n_up * tiles

    def load_slope(g):
        rows = pl.ds(pl.multiple_of((g % tiles) * TOK, TOK), TOK)
        cols = pl.ds(pl.multiple_of((g // tiles) * WIDTH, WIDTH), WIDTH)
        return pltpu.make_async_copy(slope_ref.at[rows, cols], slope.at[g % 3], slope_sem.at[g % 3])

    def load_pt(half, m):
        part = pl.ds(64 * m, 64)
        return pltpu.make_async_copy(pt_ref.at[part, half], p_t.at[part, half], pt_sem.at[half, m])

    def load_wd(j):
        rows = pl.ds(pl.multiple_of(j * WIDTH, WIDTH), WIDTH)
        return pltpu.make_async_copy(wd_ref.at[rows], wd.at[j % 2], wd_sem.at[j % 2])

    load_dz = pltpu.make_async_copy(dz_ref, dz, dz_sem)
    load_xt = pltpu.make_async_copy(xt_ref, xt, xt_sem)
    load_wd(0).start()
    load_dz.start()
    load_slope(0).start()
    load_slope(1).start()
    load_xt.start()
    load_wd(1).start()
    for half in range(2):
        for m in range(2):
            load_pt(half, m).start()
    enter(everyone)

    def axes(u):
        return [axis_of((u + n) % 3, x, y, z) for n in range(3)]

    def remote(a, b, s, r, peer):
        return pltpu.make_async_remote_copy(
            src_ref=a, dst_ref=b, send_sem=s, recv_sem=r, device_id=(peer,), device_id_type=MESH)

    def pair_copy(u):
        return remote(src.at[u % 2, :, 1 - c], pair_in.at[u % 4], pair_s.at[u % 4], pair_r.at[u % 4], partner)

    def first_copies(u):
        pos, stride = axes(u)[0]
        right = me + ((pos + 1) % 4 - pos) * stride
        left = me + ((pos + 3) % 4 - pos) * stride
        at_r, at_l, at_o = 16 * ((pos + 1) % 4), 16 * ((pos + 3) % 4), 16 * ((pos + 2) % 4)
        buf = work.at[u % 4]
        ends = [
            (at_o, opp_r.at[u], right),
            (at_o + 8, opp_l.at[u], left),
            (at_r + 8, from_l.at[u, pl.ds(8, 8)], right),
            (at_l, from_r.at[u, pl.ds(0, 8)], left),
            (at_r, from_l.at[u, pl.ds(0, 8)], right),
            (at_l + 8, from_r.at[u, pl.ds(8, 8)], left),
        ]
        return [remote(buf.at[pl.ds(at, 8)], dst, s1.at[u, n], r1.at[u, n], peer) for n, (at, dst, peer) in enumerate(ends)]

    def second_copies(u):
        pos, stride = axes(u)[1]
        return [remote(mid.at[u % 3, pl.ds(4 * ((pos + d) % 4), 4)], mid_in.at[u, d - 1], s2.at[u, d - 1], r2.at[u, d - 1],
                       me + ((pos + d) % 4 - pos) * stride) for d in range(1, 4)]

    def third_copies(u):
        pos, stride = axes(u)[2]
        return [remote(low.at[u % 3, (pos + d) % 4], low_in.at[u, d - 1], s3.at[u, d - 1], r3.at[u, d - 1],
                       me + ((pos + d) % 4 - pos) * stride) for d in range(1, 4)]

    def within(u):
        return jnp.logical_and(u >= 0, u < count)

    def produce_up(t):
        j = t // 2
        load_wd(j).wait()

        @pl.when(t == 0)
        def _():
            load_dz.wait()

        def step(i, _):
            g = j * tiles + i

            @pl.when(g + 2 < n_tiles)
            def _():
                load_slope(g + 2).start()

            load_slope(g).wait()
            rows = pl.ds(pl.multiple_of(i * TOK, TOK), TOK)
            dh = lax.dot_general(dz[rows], wd[j % 2], (((1,), (1,)), ((), ())), preferred_element_type=jnp.float32)
            d_pre[rows] = (dh * slope[g % 3]).astype(jnp.bfloat16)
            return 0

        lax.fori_loop(0, tiles, step, 0)

        @pl.when(j + 2 < n_up)
        def _():
            load_wd(j + 2).start()

        @pl.when(t == 0)
        def _():
            load_xt.wait()

        prod = jnp.dot(xt[...], d_pre[...], preferred_element_type=jnp.float32)
        src[t % 2] = prod.reshape(64, 2, ROWS, WIDTH)

    def produce_down(t):
        u = t // 2
        half = u % 2

        @pl.when(u < 2)
        def _():
            for m in range(2):
                load_pt(half, m).wait()

        cols = pl.ds(pl.multiple_of((u // 2) * 256, 256), 256)
        for m in range(2):
            rows = p_t[pl.ds(64 * m, 64), half].reshape(1024, p_t.shape[3])
            prod = jnp.dot(rows, dz[:, cols], preferred_element_type=jnp.float32)
            prod = prod.reshape(32, 2, 2, ROWS, 256)
            src[t % 2, pl.ds(32 * m, 32), :, :, 0:256] = prod[:, :, 0]
            src[t % 2, pl.ds(32 * m, 32), :, :, 256:512] = prod[:, :, 1]

    def body(t, _):
        @pl.when(jnp.logical_and(t % 2 == 0, t < count))
        def _():
            produce_up(t)

        @pl.when(jnp.logical_and(t % 2 == 1, t < count))
        def _():
            produce_down(t)

        @pl.when(t < count)
        def _():
            pair_copy(t).start()

        uc = t - 3

        @pl.when(within(uc))
        def _():
            copies = first_copies(uc)
            (pos, _), _, _ = axes(uc)
            at_r, at_l = 16 * ((pos + 1) % 4), 16 * ((pos + 3) % 4)
            copies[0].wait_recv()
            work[uc % 4, pl.ds(at_r, 8)] += opp_r[uc]
            copies[4].start()
            copies[1].wait_recv()
            work[uc % 4, pl.ds(at_l + 8, 8)] += opp_l[uc]
            copies[5].start()

        ud = t - 5

        @pl.when(within(ud))
        def _():
            copies = first_copies(ud)
            for copy in copies[2:]:
                copy.wait_recv()
            (pos, _), _, _ = axes(ud)
            for n in range(0, 16, 4):
                mid[ud % 3, pl.ds(n, 4)] = (work[ud % 4, pl.ds(16 * pos + n, 4)] + from_l[ud, pl.ds(n, 4)]) + from_r[ud, pl.ds(n, 4)]
            for copy in second_copies(ud):
                copy.start()
            for copy in copies:
                copy.wait_send()

        ub = t - 1

        @pl.when(within(ub))
        def _():
            copy = pair_copy(ub)
            copy.wait_recv()
            (_, st1), (_, st2), (_, st3) = axes(ub)

            def add(b, _):
                for q in range(4):
                    for n in range(4):
                        here = b * (st1 // 2) + q * (st2 // 2) + n * (st3 // 2)
                        work[ub % 4, 16 * b + 4 * q + n] = src[ub % 2, here, c] + pair_in[ub % 4, here]
                return 0

            lax.fori_loop(0, 4, add, 0)
            copy.wait_send()
            for copy in first_copies(ub)[:4]:
                copy.start()

        ue = t - 7

        @pl.when(within(ue))
        def _():
            copies = second_copies(ue)
            for copy in copies:
                copy.wait_recv()
            _, (pos, _), _ = axes(ue)
            low[ue % 3] = (mid[ue % 3, pl.ds(4 * pos, 4)] + mid_in[ue, 0]) + (mid_in[ue, 1] + mid_in[ue, 2])
            for copy in third_copies(ue):
                copy.start()
            for copy in copies:
                copy.wait_send()

        uf = t - 9

        @pl.when(within(uf))
        def _():
            copies = third_copies(uf)
            for copy in copies:
                copy.wait_recv()
            _, _, (pos, _) = axes(uf)
            total = (low[uf % 3, pos] + low_in[uf, 0]) + (low_in[uf, 1] + low_in[uf, 2])

            @pl.when(uf % 2 == 0)
            def _():
                out_up[:, pl.ds(pl.multiple_of((uf // 2) * WIDTH, WIDTH), WIDTH)] = total

            @pl.when(uf % 2 == 1)
            def _():
                tile = uf // 2
                cols = pl.ds(pl.multiple_of((tile // 2) * 256, 256), 256)
                out_down[2 * (tile % 2), :, cols] = total[:, 0:256]
                out_down[2 * (tile % 2) + 1, :, cols] = total[:, 256:512]

            for copy in copies:
                copy.wait_send()

        return 0

    lax.fori_loop(0, count + 9, body, 0)


def backward(slope, d_out, w_down, tok_cols, act_rows):
    tokens, hidden = slope.shape
    model = d_out.shape[1]
    n_up, n_down = hidden // WIDTH, 2 * (model // 256)
    count = n_up + n_down
    f32, bf16 = jnp.float32, jnp.bfloat16
    block = (ROWS, WIDTH)
    dma = pltpu.SemaphoreType.DMA
    out_up, out_down = pl.pallas_call(
        functools.partial(backward_kernel, n_up, n_down),
        out_shape=(jax.ShapeDtypeStruct((ROWS, hidden), f32), jax.ShapeDtypeStruct((4, ROWS, model), f32)),
        in_specs=[pl.BlockSpec(memory_space=pl.ANY)] * 5,
        out_specs=(pl.BlockSpec(memory_space=pltpu.VMEM), pl.BlockSpec(memory_space=pltpu.VMEM)),
        scratch_shapes=[
            pltpu.VMEM((model, tokens), bf16),
            pltpu.VMEM((tokens, model), bf16),
            pltpu.VMEM((hidden // 32, 2, 16, tokens), bf16),
            pltpu.VMEM((3, TOK, WIDTH), f32),
            pltpu.VMEM((2, WIDTH, model), bf16),
            pltpu.VMEM((tokens, WIDTH), bf16),
            pltpu.VMEM((2, 64, 2) + block, f32),
            pltpu.VMEM((4, 64) + block, f32),
            pltpu.VMEM((4, 64) + block, f32),
            pltpu.VMEM((count, 8) + block, f32),
            pltpu.VMEM((count, 8) + block, f32),
            pltpu.VMEM((count, 16) + block, f32),
            pltpu.VMEM((count, 16) + block, f32),
            pltpu.VMEM((3, 16) + block, f32),
            pltpu.VMEM((count, 3, 4) + block, f32),
            pltpu.VMEM((3, 4) + block, f32),
            pltpu.VMEM((count, 3) + block, f32),
            dma, dma, dma((2, 2)), dma((3,)), dma((2,)), dma((4,)), dma((4,)),
            dma((count, 6)), dma((count, 6)), dma((count, 3)), dma((count, 3)), dma((count, 3)), dma((count, 3)),
        ],
        compiler_params=pltpu.CompilerParams(collective_id=1, has_side_effects=True, vmem_limit_bytes=VMEM_BYTES),
    )(slope, d_out, w_down, tok_cols, act_rows)
    return out_up, out_down.reshape(hidden // 128, model)


def solution(mesh):
    group_size = mesh.shape['data']

    def local_step(tok_rows, w_up, w_down, heads, label_rows):
        total_rows = tok_rows.shape[0] * group_size
        by_class = heads.transpose(2, 0, 1)
        slope, act_rows, tok_cols, logits = forward(tok_rows, w_up, w_down, by_class)
        mix_wts, d_out = solve_weights(logits, label_rows, by_class, total_rows)
        up_shard, down_shard = backward(slope, d_out, w_down, tok_cols, act_rows)
        return mix_wts, up_shard, down_shard

    return jax.shard_map(local_step, mesh=mesh, in_specs=(P('data', None), P(), P(), P(), P(None, 'data')), out_specs=(P(), P('data', None), P('data', None)), check_vma=False)
```
